32 devices in a mesh: bits: 32 (over z, y, x, core).
Axes of the slice: x: 2, y: 2, z: 4, core: 2. Of those that a mesh axis runs over, the one named last changes fastest.
Arguments:
- environment: float32 [2, 128, 64, 4096], P(None, 'bits'), may hold values from -6 to 6
- peps: float32 [2, 2, 8, 8, 8, 8], replicated, may hold values from -2 to 2
- operators: float32 [2, 2, 2], replicated, may hold values from -4 to 4
- gauge: float32 [128, 128], replicated, may hold values from -0.5 to 0.5
Outputs:
- absorbed: float32 [2, 128, 262144], P(None, None, 'bits')
- rms: float32 [2], replicated
The draws below stay inside these ranges and needn't reach their ends.
All inputs are finite; a program needn't handle non-finite values.
Results may differ from the reference program's by a relative error of at most 0.0003.
Values sent between devices are 32-bit elements; how exact they have to be, the bound alone decides.
A program may use at most 512 MiB of HBM per device.

```python
import jax
import jax.numpy as jnp
from jax import lax

D = 8
PHYS = 2
CHI = 128
COLS = 2
NENV = 2
LEGS = 4096


def draw_peps(key, part):
    first, second = jax.random.split(jax.random.fold_in(key, 17), 2)
    shape = (COLS, PHYS, D, D, D, D)
    base = jax.random.truncated_normal(first, -4.0, 4.0, shape, jnp.float32)
    ramp = 3.0 ** (jnp.arange(D, dtype=jnp.float32) / (D - 1))
    rough = jnp.exp(jax.random.uniform(second, (COLS, 1, 1, 1, 1, D), jnp.float32, -0.2, 0.2))
    return (base / D * ramp * rough).astype(jnp.float32)


def levels(own_key, dims, shards, low, largest):
    loudness = 1.0
    for axis_at, parts in shards:
        draws = jax.random.uniform(jax.random.fold_in(jax.random.fold_in(own_key, 6), axis_at), (parts,), jnp.float32, low / len(shards), largest / len(shards))
        loudness = loudness * jnp.repeat(jnp.exp(draws), dims[axis_at] // parts).reshape((-1,) + (1,) * (len(dims) - 1 - axis_at))
    return loudness


def noise(stream_key, dims, spread, most, pieces=(), kind=jnp.bfloat16):
    entries = spread * jax.random.normal(stream_key, dims, jnp.float32)
    if pieces:
        entries = entries * levels(stream_key, dims, pieces, -0.22, 0.18)
    return jnp.clip(entries, -most, most).astype(kind)


def setup_inputs(seed: int = 0) -> dict:
    streams_of = jax.random.split(jax.random.key(seed), 5)
    environment = noise(streams_of[0], (NENV, CHI, D * D, LEGS), 1.0, 6.0, ((1, 32),), jnp.float32)
    peps = draw_peps(jax.random.fold_in(streams_of[4], 71), 0)
    operators = noise(streams_of[2], (COLS, PHYS, PHYS), 1.0, 4.0, (), jnp.float32)
    gauge = noise(streams_of[3], (CHI, CHI), CHI ** -0.5, 0.5, (), jnp.float32)
    return {"environment": environment, "peps": peps, "operators": operators, "gauge": gauge}


EPS = 1e-06

def absorb(state, peps, operators):
    count, rows = (state.shape[0], state.shape[1])
    width = peps.shape[2]
    columns = peps.shape[0]
    for column in range(columns):
        before = width ** (2 * column)
        after = width ** (2 * (columns - 1 - column))
        view = state.reshape(count, rows, width, width, before, width, width, after)
        bra_side = jnp.einsum('pq,qbvms->pbvms', operators[column], peps[column], precision=lax.Precision.HIGHEST)
        partial_value = jnp.einsum('eclbzuvx,plukr->ecrpbzkvx', view, peps[column], precision=lax.Precision.HIGHEST)
        state = jnp.einsum('ecrpbzkvx,pbvms->ecrszkmx', partial_value, bra_side, precision=lax.Precision.HIGHEST)
    return state.reshape(count, rows, -1)

def reference(environment, peps, operators, gauge):

    def single(block):
        grown = absorb(block[None], peps, operators)[0]
        return jnp.dot(gauge, grown, precision=lax.Precision.HIGHEST, preferred_element_type=jnp.float32)
    gauged = lax.map(single, environment)
    mean = lax.optimization_barrier(jnp.mean(gauged * gauged, axis=(1, 2)))
    absorbed = gauged * lax.rsqrt(mean + EPS)[:, None, None]
    return (absorbed, jnp.sqrt(mean))
```

```python
import functools

import jax
import jax.numpy as jnp
from jax import lax
from jax.experimental import pallas as pl
from jax.experimental.pallas import tpu as pltpu
from jax.sharding import PartitionSpec as P

EPS = 1e-06
LANES = 128
GROUP = 4
PITCH_PAD = 8


def split_rows(value):
    high = value.astype(jnp.bfloat16)
    low = (value - high.astype(jnp.float32)).astype(jnp.bfloat16)
    return jnp.concatenate([high, high, low], axis=0)


def split_weights(value):
    high = lax.reduce_precision(value, 8, 7)
    low = value - high
    return jnp.concatenate([high, low, high], axis=1).astype(jnp.bfloat16)


def product(weights, value):
    return jnp.dot(weights, split_rows(value), preferred_element_type=jnp.float32)


def exchange_halves(first, second):
    half = LANES // 2
    lower = lax.broadcasted_iota(jnp.int32, first.shape, 1) < half
    return (
        jnp.where(lower, first, pltpu.roll(second, half, 1)),
        jnp.where(lower, pltpu.roll(first, half, 1), second),
    )


def absorb_kernel(w, rows, x_ref, ket0, bra0, ket1, bra1, out_ref, source, wide, middle, turn):
    square = w * w
    pitch = 2 * square + PITCH_PAD
    legs = x_ref.shape[2]
    step = legs // w
    pieces = step // LANES

    def fill(pair, block, value):
        wide[pl.ds(pl.multiple_of((pair * square + block) * pitch, 8), 2 * square), :] = value

    def gather(row, carry):
        for piece in range(w * pieces):
            source[pl.ds(pl.multiple_of((row * w * pieces + piece) * square, 8), square), :] = x_ref[
                row, :, piece * LANES:(piece + 1) * LANES
            ]
        return carry

    lax.fori_loop(0, x_ref.shape[0], gather, 0)

    def first(bond, carry):
        columns = []
        for pair in range(2):
            for piece in range(pieces):
                taken = []
                for row in (2 * pair, 2 * pair + 1):
                    taken.append(jnp.concatenate([
                        source[pl.ds(((row * w + leg) * pieces + piece) * square + bond, w, stride=w), :]
                        for leg in range(w)
                    ], axis=0))
                columns += exchange_halves(*taken)
        result = product(ket0[...], jnp.concatenate(columns, axis=1))
        for at in range(2 * w):
            fill(at // w, bond * w + at % w, result[:, at * LANES:(at + 1) * LANES])
        return carry

    def turned(bra, bond):
        columns = []
        for leg in range(w):
            for pair in range(2):
                columns.append(jnp.concatenate([
                    wide[pl.ds(pair * square * pitch + p * square + bond * w + leg, square, stride=pitch), :]
                    for p in range(2)
                ], axis=0))
        result = product(bra[...], jnp.concatenate(columns, axis=1))
        for out in range(w):
            block = jnp.concatenate([
                result[out * w:(out + 1) * w, (leg * 2 + pair) * LANES:(leg * 2 + pair + 1) * LANES]
                for pair in range(2) for leg in range(w)
            ], axis=0)
            yield out, block.T

    def second(bond, carry):
        for out, block in turned(bra0, bond):
            middle[pl.ds(pl.multiple_of((bond * w + out) * LANES, 8), LANES), :] = block
        return carry

    def third(bond, carry):
        columns = []
        for pair in range(2):
            for leg in range(w):
                columns.append(jnp.concatenate([
                    middle[pl.ds((other * w + bond) * LANES + pair * square + leg, w, stride=w), :]
                    for other in range(w)
                ], axis=0))
        result = product(ket1[...], jnp.concatenate(columns, axis=1))
        for at in range(2 * w):
            fill(at // w, bond * w + at % w, result[:, at * LANES:(at + 1) * LANES])
        return carry

    per_bond = legs // LANES
    part, blk = (out_ref.shape[2], out_ref.shape[3])

    def fourth(bond, carry):
        for out, block in turned(bra1, bond):
            turn[out] = block
            even = turn[out, pl.ds(0, square, stride=2), :]
            odd = turn[out, pl.ds(1, square, stride=2), :]
            for low, value in enumerate(exchange_halves(even, odd)):
                for pair in range(2):
                    row = pair * 2 + low
                    if row >= rows:
                        continue
                    for sub in range(per_bond // blk):
                        at = (bond * w + out) * (per_bond // blk) + sub
                        begin = pair * per_bond + sub * blk
                        out_ref[at // part, row, at % part] = value[begin:begin + blk]
        return carry

    for stage in (first, second, third, fourth):
        lax.fori_loop(0, w, stage, 0)


def absorb(x, kets, bras, devices):
    rows, square, legs = x.shape
    w = kets[0].shape[0] // 2
    w = int(round(w ** 0.5))
    if rows < GROUP:
        x = jnp.pad(x, ((0, GROUP - rows), (0, 0), (0, 0)))
    share = square * legs // devices // LANES
    blk = min(share, legs // LANES)
    pitch = 2 * square + PITCH_PAD
    return pl.pallas_call(
        functools.partial(absorb_kernel, w, rows),
        out_shape=jax.ShapeDtypeStruct((devices, rows, share // blk, blk, LANES), jnp.float32),
        in_specs=[pl.BlockSpec(memory_space=pltpu.VMEM)] * 5,
        out_specs=pl.BlockSpec(memory_space=pltpu.VMEM),
        scratch_shapes=[
            pltpu.VMEM((GROUP * square * legs // LANES, LANES), jnp.float32),
            pltpu.VMEM((2 * square * pitch, LANES), jnp.float32),
            pltpu.VMEM((square * LANES, LANES), jnp.float32),
            pltpu.VMEM((w, LANES, LANES), jnp.float32),
        ],
        compiler_params=pltpu.CompilerParams(vmem_limit_bytes=48 * 1024 * 1024),
        cost_estimate=pl.CostEstimate(flops=2 * 10 ** 10, bytes_accessed=8 * rows * square * legs, transcendentals=0),
        name="absorb",
    )(x, kets[0], bras[0], kets[1], bras[1])


def gauge_kernel(got_ref, gauge_ref, out_ref, sums_ref):
    chi, share, lanes = got_ref.shape
    step = min(share, 8)

    def some(at, total):
        value = jnp.concatenate([got_ref[:, at * step + i, :] for i in range(step)], axis=1)
        result = product(gauge_ref[...], value)
        out_ref[:, pl.ds(pl.multiple_of(at * step * lanes, lanes), step * lanes)] = result
        return total + jnp.sum(result * result, axis=0, keepdims=True)

    total = lax.fori_loop(0, share // step, some, jnp.zeros((1, step * lanes), jnp.float32))
    sums_ref[...] = total


def apply_gauge(got, gauge):
    chi, share, lanes = got.shape
    return pl.pallas_call(
        gauge_kernel,
        out_shape=(
            jax.ShapeDtypeStruct((chi, share * lanes), jnp.float32),
            jax.ShapeDtypeStruct((1, min(share, 8) * lanes), jnp.float32),
        ),
        in_specs=[pl.BlockSpec(memory_space=pltpu.VMEM)] * 2,
        out_specs=(pl.BlockSpec(memory_space=pltpu.VMEM),) * 2,
        compiler_params=pltpu.CompilerParams(vmem_limit_bytes=32 * 1024 * 1024),
        cost_estimate=pl.CostEstimate(flops=10 ** 9, bytes_accessed=8 * chi * share * lanes, transcendentals=0),
        name="gauge",
    )(got, gauge)


def body(environment, peps, operators, gauge):
    count, rows, square, legs = environment.shape
    devices = lax.axis_size("bits")
    bra = jnp.einsum("jpq,jqbvms->jsmpbv", operators, peps, precision="highest")
    orders = ((0, 4, 3, 2, 1), (0, 4, 3, 1, 2))
    kets = [split_weights(peps[j].transpose(orders[j]).reshape(2 * square, square)) for j in range(2)]
    bras = [split_weights(bra[j].reshape(square, 2 * square)) for j in range(2)]
    weights = split_weights(gauge)
    chi = rows * devices
    gauged, means = [], []
    entries = chi * square * legs
    for e in range(count):
        grown = absorb(environment[e], kets, bras, devices)
        got = lax.all_to_all(grown, "bits", 0, 0, tiled=True)
        value, sums = apply_gauge(got.reshape(chi, -1, LANES), weights)
        gauged.append(value)
        means.append(jnp.sum(sums))
    mean = lax.psum(jnp.stack(means), "bits") / entries
    scale = lax.rsqrt(mean + EPS)
    absorbed = jnp.stack([gauged[e] * scale[e] for e in range(count)])
    return (absorbed, jnp.sqrt(mean))


def solution(mesh):
    placed = (P(None, "bits", None, None), P(), P(), P())
    return jax.shard_map(
        body, mesh=mesh, in_specs=placed, out_specs=(P(None, None, "bits"), P()), check_vma=False
    )
```

```python
import functools

import jax
import jax.numpy as jnp
from jax import lax
from jax.experimental import pallas as pl
from jax.experimental.pallas import tpu as pltpu
from jax.sharding import PartitionSpec as P

EPS = 1e-06
LANES = 128
GROUP = 4
PITCH_PAD = 8


def split_rows(value):
    high = value.astype(jnp.bfloat16)
    low = (value - high.astype(jnp.float32)).astype(jnp.bfloat16)
    return jnp.concatenate([high, high, low], axis=0)


def split_weights(value):
    high = lax.reduce_precision(value, 8, 7)
    low = value - high
    return jnp.concatenate([high, low, high], axis=1).astype(jnp.bfloat16)


def product(weights, value):
    return jnp.dot(weights, split_rows(value), preferred_element_type=jnp.float32)


def exchange_halves(first, second):
    half = LANES // 2
    lower = lax.broadcasted_iota(jnp.int32, first.shape, 1) < half
    return (
        jnp.where(lower, first, pltpu.roll(second, half, 1)),
        jnp.where(lower, pltpu.roll(first, half, 1), second),
    )


def absorb_kernel(w, rows, x_ref, ket0, bra0, ket1, bra1, out_ref, source, wide, middle, turn):
    square = w * w
    pitch = 2 * square + PITCH_PAD
    legs = x_ref.shape[2]
    step = legs // w
    pieces = step // LANES

    def fill(pair, block, value):
        wide[pl.ds(pl.multiple_of((pair * square + block) * pitch, 8), 2 * square), :] = value

    def gather(row, carry):
        for piece in range(w * pieces):
            source[pl.ds(pl.multiple_of((row * w * pieces + piece) * square, 8), square), :] = x_ref[
                row, :, piece * LANES:(piece + 1) * LANES
            ]
        return carry

    lax.fori_loop(0, rows, gather, 0)
    if rows < GROUP:
        unused = (GROUP - rows) * square * w * pieces
        source[rows * square * w * pieces:, :] = jnp.zeros((unused, LANES), jnp.float32)

    def first(bond, carry):
        columns = []
        for pair in range(2):
            for piece in range(pieces):
                taken = []
                for row in (2 * pair, 2 * pair + 1):
                    taken.append(jnp.concatenate([
                        source[pl.ds(((row * w + leg) * pieces + piece) * square + bond, w, stride=w), :]
                        for leg in range(w)
                    ], axis=0))
                columns += exchange_halves(*taken)
        result = product(ket0[...], jnp.concatenate(columns, axis=1))
        for at in range(2 * w):
            fill(at // w, bond * w + at % w, result[:, at * LANES:(at + 1) * LANES])
        return carry

    def turned(bra, bond):
        columns = []
        for leg in range(w):
            for pair in range(2):
                columns.append(jnp.concatenate([
                    wide[pl.ds(pair * square * pitch + p * square + bond * w + leg, square, stride=pitch), :]
                    for p in range(2)
                ], axis=0))
        result = product(bra[...], jnp.concatenate(columns, axis=1))
        for out in range(w):
            block = jnp.concatenate([
                result[out * w:(out + 1) * w, (leg * 2 + pair) * LANES:(leg * 2 + pair + 1) * LANES]
                for pair in range(2) for leg in range(w)
            ], axis=0)
            yield out, block.T

    def second(bond, carry):
        for out, block in turned(bra0, bond):
            middle[pl.ds(pl.multiple_of((bond * w + out) * LANES, 8), LANES), :] = block
        return carry

    def third(bond, carry):
        columns = []
        for pair in range(2):
            for leg in range(w):
                columns.append(jnp.concatenate([
                    middle[pl.ds((other * w + bond) * LANES + pair * square + leg, w, stride=w), :]
                    for other in range(w)
                ], axis=0))
        result = product(ket1[...], jnp.concatenate(columns, axis=1))
        for at in range(2 * w):
            fill(at // w, bond * w + at % w, result[:, at * LANES:(at + 1) * LANES])
        return carry

    per_bond = legs // LANES
    part, blk = (out_ref.shape[2], out_ref.shape[3])

    def fourth(bond, carry):
        for out, block in turned(bra1, bond):
            turn[out] = block
            even = turn[out, pl.ds(0, square, stride=2), :]
            odd = turn[out, pl.ds(1, square, stride=2), :]
            for low, value in enumerate(exchange_halves(even, odd)):
                for pair in range(2):
                    row = pair * 2 + low
                    if row >= rows:
                        continue
                    for sub in range(per_bond // blk):
                        at = (bond * w + out) * (per_bond // blk) + sub
                        begin = pair * per_bond + sub * blk
                        out_ref[at // part, row, at % part] = value[begin:begin + blk]
        return carry

    for stage in (first, second, third, fourth):
        lax.fori_loop(0, w, stage, 0)


def absorb(environment, e, kets, bras, devices):
    rows, square, legs = environment.shape[1:]
    w = kets[0].shape[0] // 2
    w = int(round(w ** 0.5))
    share = square * legs // devices // LANES
    blk = min(share, legs // LANES)
    pitch = 2 * square + PITCH_PAD
    return pl.pallas_call(
        functools.partial(absorb_kernel, w, rows),
        out_shape=jax.ShapeDtypeStruct((devices, rows, share // blk, blk, LANES), jnp.float32),
        grid=(1,),
        in_specs=[pl.BlockSpec((None, rows, square, legs), lambda i: (e, 0, 0, 0))]
        + [pl.BlockSpec(memory_space=pltpu.VMEM)] * 4,
        out_specs=pl.BlockSpec(memory_space=pltpu.VMEM),
        scratch_shapes=[
            pltpu.VMEM((GROUP * square * legs // LANES, LANES), jnp.float32),
            pltpu.VMEM((2 * square * pitch, LANES), jnp.float32),
            pltpu.VMEM((square * LANES, LANES), jnp.float32),
            pltpu.VMEM((w, LANES, LANES), jnp.float32),
        ],
        compiler_params=pltpu.CompilerParams(vmem_limit_bytes=48 * 1024 * 1024),
        cost_estimate=pl.CostEstimate(flops=2 * 10 ** 10, bytes_accessed=8 * rows * square * legs, transcendentals=0),
        name="absorb",
    )(environment, kets[0], bras[0], kets[1], bras[1])


def gauge_kernel(got_ref, gauge_ref, out_ref, sums_ref):
    chi, share, lanes = got_ref.shape
    step = min(share, 8)

    def some(at, total):
        value = jnp.concatenate([got_ref[:, at * step + i, :] for i in range(step)], axis=1)
        result = product(gauge_ref[...], value)
        out_ref[:, pl.ds(pl.multiple_of(at * step * lanes, lanes), step * lanes)] = result
        return total + jnp.sum(result * result, axis=0, keepdims=True)

    total = lax.fori_loop(0, share // step, some, jnp.zeros((1, step * lanes), jnp.float32))
    sums_ref[...] = total


def apply_gauge(got, gauge):
    chi, share, lanes = got.shape
    return pl.pallas_call(
        gauge_kernel,
        out_shape=(
            jax.ShapeDtypeStruct((chi, share * lanes), jnp.float32),
            jax.ShapeDtypeStruct((1, min(share, 8) * lanes), jnp.float32),
        ),
        in_specs=[pl.BlockSpec(memory_space=pltpu.VMEM)] * 2,
        out_specs=(pl.BlockSpec(memory_space=pltpu.VMEM),) * 2,
        compiler_params=pltpu.CompilerParams(vmem_limit_bytes=32 * 1024 * 1024),
        cost_estimate=pl.CostEstimate(flops=10 ** 9, bytes_accessed=8 * chi * share * lanes, transcendentals=0),
        name="gauge",
    )(got, gauge)


def body(environment, peps, operators, gauge):
    count, rows, square, legs = environment.shape
    devices = lax.axis_size("bits")
    bra = jnp.einsum("jpq,jqbvms->jsmpbv", operators, peps, precision="highest")
    orders = ((0, 4, 3, 2, 1), (0, 4, 3, 1, 2))
    kets = [split_weights(peps[j].transpose(orders[j]).reshape(2 * square, square)) for j in range(2)]
    bras = [split_weights(bra[j].reshape(square, 2 * square)) for j in range(2)]
    weights = split_weights(gauge)
    chi = rows * devices
    gauged, means = [], []
    entries = chi * square * legs
    for e in range(count):
        grown = absorb(environment, e, kets, bras, devices)
        got = lax.all_to_all(grown, "bits", 0, 0, tiled=True)
        value, sums = apply_gauge(got.reshape(chi, -1, LANES), weights)
        gauged.append(value)
        means.append(jnp.sum(sums))
    copies = jnp.broadcast_to(jnp.stack(means)[None], (devices, count))
    mean = jnp.sum(lax.all_to_all(copies, "bits", 0, 0, tiled=True), axis=0) / entries
    scale = lax.rsqrt(mean + EPS)
    absorbed = jnp.stack([gauged[e] * scale[e] for e in range(count)])
    return (absorbed, jnp.sqrt(mean))


def solution(mesh):
    placed = (P(None, "bits", None, None), P(), P(), P())
    return jax.shard_map(
        body, mesh=mesh, in_specs=placed, out_specs=(P(None, None, "bits"), P()), check_vma=False
    )
```
